32 devices in a mesh: sp: 16 (over z, x, core), tp: 2 (over y).
Axes of the slice: x: 2, y: 2, z: 4, core: 2. Of those that a mesh axis runs over, the one named last changes fastest.
Arguments:
- leak_rate: float32 [2, 32768, 1024], P(None, 'sp', 'tp'), may hold values from 0.2 to 2
- signal_in: bfloat16 [2, 32768, 1024], P(None, 'sp', 'tp'), may hold values from -6 to 6
- gate_in: bfloat16 [2, 32768, 1024], P(None, 'sp', 'tp'), may hold values from -6 to 6
Outputs:
- sequence_out: bfloat16 [2, 32768, 1024], P(None, 'sp', 'tp')
The draws below stay inside these ranges and needn't reach their ends.
All inputs are finite; a program needn't handle non-finite values.
Results may differ from the reference program's by a relative error of at most 0.0017.
Values sent between devices are 32-bit elements; how exact they have to be, the bound alone decides.
A program may use at most 192 MiB of HBM per device.

```python
import jax
import jax.numpy as jnp
from jax import lax

BATCH = 2
CHANNELS = 1024
LENGTH = 32768


def steps_of(stream_key, dims, pieces, low, largest):
    factor_of = 1.0
    for axis_at, shards_of in pieces:
        heights = jax.random.uniform(jax.random.fold_in(jax.random.fold_in(stream_key, 6), axis_at), (shards_of,), jnp.float32, low / len(pieces), largest / len(pieces))
        factor_of = factor_of * jnp.repeat(jnp.exp(heights), dims[axis_at] // shards_of).reshape((-1,) + (1,) * (len(dims) - 1 - axis_at))
    return factor_of


def centred(key, shape, scale, limit, pieces=(), kind=jnp.bfloat16):
    factor_of = steps_of(key, shape, pieces, -0.22, 0.18) if pieces else 1.0
    result = jax.random.normal(key, shape, jnp.float32) * scale * factor_of
    return jnp.minimum(jnp.maximum(result, -limit), limit).astype(kind)


def setup_inputs(seed: int = 0) -> dict:
    splits = jax.random.split(jax.random.key(seed), 4)
    leak_rate = jnp.clip(0.2 + 1.8 * jax.random.uniform(splits[0], (BATCH, LENGTH, CHANNELS), jnp.float32) ** steps_of(splits[0], (BATCH, LENGTH, CHANNELS), ((1, 16), (2, 2)), -0.2, 0.2), 0.2, 2.0)
    signal_in = centred(splits[1], (BATCH, LENGTH, CHANNELS), 1.0, 6.0, ((1, 16), (2, 2)))
    gate_in = centred(splits[2], (BATCH, LENGTH, CHANNELS), 1.0, 6.0, ((1, 16), (2, 2)))
    return dict(leak_rate=leak_rate, signal_in=signal_in, gate_in=gate_in)


def join_pair(earlier, later):
    return earlier[0] * later[0], later[0] * earlier[1] + later[1]


def reference(leak_rate, signal_in, gate_in):
    keep = jnp.exp(-leak_rate / LENGTH)
    push = signal_in.astype(jnp.float32) * LENGTH ** -0.5
    forward = lax.associative_scan(join_pair, (keep, push), axis=1)[1]
    backward = lax.associative_scan(join_pair, (keep, push), axis=1, reverse=True)[1]
    states = forward + backward
    gated = states * jax.nn.sigmoid(gate_in.astype(jnp.float32))
    sequence_out = gated.astype(jnp.bfloat16)
    return sequence_out
```

```python
import functools
import math

import jax
import jax.numpy as jnp
from jax import lax
from jax.experimental import pallas as pl
from jax.experimental.pallas import tpu as pltpu
from jax.sharding import PartitionSpec as P

F32, BF16 = jnp.float32, jnp.bfloat16
VMEM = pltpu.VMEM
MIB = 1 << 20


def chunk_copy(hbm, vmem, sem, j, rows):
    at = pl.ds(pl.multiple_of(j * rows, rows), rows)
    return pltpu.make_async_copy(hbm.at[:, at, :], vmem.at[:, at, :], sem.at[j])


def local_kernel(
    total_length, rows, leak_hbm, signal_hbm, gate_hbm,
    mixed_ref, from_left_ref, from_right_ref, block_ref, message_ref,
    leak, signal, gate, leak_sem, signal_sem, gate_sem,
):
    batch, length, channels = leak.shape
    blocks = length // rows
    rate = math.log2(math.e) / total_length
    half_scale = 0.5 * total_length ** -0.5

    def start(j, _):
        chunk_copy(leak_hbm, leak, leak_sem, j, rows).start()
        chunk_copy(signal_hbm, signal, signal_sem, j, rows).start()
        chunk_copy(gate_hbm, gate, gate_sem, j, rows).start()
        return _

    lax.fori_loop(0, blocks, start, 0)

    row = lax.broadcasted_iota(jnp.int32, (rows, 2 * rows), 0)
    col = lax.broadcasted_iota(jnp.int32, (rows, 2 * rows), 1) % rows
    upto = jnp.where(row >= col, 1.0, 0.0).astype(BF16)
    onward = jnp.where(row <= col, 1.0, 0.0).astype(BF16)
    once = upto[:, :rows]

    def step(j, carry):
        chunk_copy(leak_hbm, leak, leak_sem, j, rows).wait()
        chunk_copy(signal_hbm, signal, signal_sem, j, rows).wait()
        chunk_copy(gate_hbm, gate, gate_sem, j, rows).wait()
        at = pl.ds(pl.multiple_of(j * rows, rows), rows)
        new = []
        for b in range(batch):
            lk = leak[b, at, :]
            x = signal[b, at, :]
            xf = x.astype(F32)
            upto_here = jnp.dot(once, lk.astype(BF16), preferred_element_type=F32) * rate
            before = upto_here - lk * rate
            low_f = ((jnp.exp2(upto_here) - 1.0) * xf).astype(BF16)
            low_b = ((jnp.exp2(-before) - 1.0) * xf).astype(BF16)
            sum_f = jnp.dot(upto, jnp.concatenate([x, low_f], 0), preferred_element_type=F32)
            sum_b = jnp.dot(onward, jnp.concatenate([x, low_b], 0), preferred_element_type=F32)
            u = jnp.exp2(-upto_here)
            v = jnp.exp2(before)
            gated = half_scale + half_scale * jnp.tanh(gate[b, at, :].astype(F32) * 0.5)
            fwd = u * sum_f
            bwd = v * sum_b
            mixed_ref[b, at, :] = (fwd + bwd) * gated
            from_left_ref[b, at, :] = u * gated
            from_right_ref[b, at, :] = v * gated
            leaked = jnp.sum(lk, axis=0, keepdims=True)
            end_f, end_b = fwd[rows - 1 :], bwd[:1]
            block_ref[j, pl.ds(b, 1), :] = leaked
            block_ref[j, pl.ds(batch + b, 1), :] = end_f
            block_ref[j, pl.ds(2 * batch + b, 1), :] = end_b
            all_leaked, all_f, all_b = carry[b]
            new.append((
                all_leaked + leaked,
                jnp.exp2(-rate * leaked) * all_f + end_f,
                all_b + jnp.exp2(-rate * all_leaked) * end_b,
            ))
        return tuple(new)

    zero = jnp.zeros((1, channels), F32)
    final = lax.fori_loop(0, blocks, step, ((zero, zero, zero),) * batch)
    for b in range(batch):
        all_leaked, all_f, all_b = final[b]
        message_ref[0, pl.ds(b, 1), :] = all_leaked
        message_ref[1, pl.ds(b, 1), :] = all_leaked
        message_ref[0, pl.ds(batch + b, 1), :] = all_f
        message_ref[1, pl.ds(batch + b, 1), :] = all_b


def exchange_kernel(total_length, n, message_ref, enter_ref, held, send_sem, recv_sem):
    me = lax.axis_index("sp")
    batch = message_ref.shape[1] // 2
    rate = math.log2(math.e) / total_length
    barrier = pltpu.get_barrier_semaphore()
    for d in range(1, n):
        pl.semaphore_signal(
            barrier, inc=1, device_id={"sp": lax.rem(me + d, n)}, device_id_type=pl.DeviceIdType.MESH
        )
    pl.semaphore_wait(barrier, n - 1)
    copies = []
    for d in range(1, n):
        side = jnp.where(me + d < n, 0, 1)
        copies.append(pltpu.make_async_remote_copy(
            src_ref=message_ref.at[side],
            dst_ref=held.at[d],
            send_sem=send_sem.at[d],
            recv_sem=recv_sem.at[d],
            device_id={"sp": lax.rem(me + d, n)},
            device_id_type=pl.DeviceIdType.MESH,
        ))
        copies[-1].start()
    for copy in copies:
        copy.wait()
    zero = jnp.zeros((batch,) + message_ref.shape[2:], F32)
    state_f, state_b, passed_f, passed_b = zero, zero, zero, zero
    for d in range(1, n):
        got = held[d]
        state_f = jnp.where(me >= d, state_f + jnp.exp2(-rate * passed_f) * got[batch:], state_f)
        passed_f = passed_f + got[:batch]
        got = held[n - d]
        state_b = jnp.where(me + d < n, state_b + jnp.exp2(-rate * passed_b) * got[batch:], state_b)
        passed_b = passed_b + got[:batch]
    enter_ref[0] = state_f
    enter_ref[1] = state_b


def finish_kernel(
    total_length, rows, mixed_ref, from_left_ref, from_right_ref, block_ref, enter_ref,
    out_hbm, out, left, right, out_sem,
):
    batch, length, channels = out.shape
    blocks = length // rows
    rate = math.log2(math.e) / total_length

    def carry(k, states):
        state_f, state_b = states
        left[k] = state_f
        state_f = jnp.exp2(-rate * block_ref[k, :batch]) * state_f + block_ref[k, batch : 2 * batch]
        j = blocks - 1 - k
        state_b = jnp.exp2(-rate * block_ref[j, :batch]) * state_b
        right[j] = state_b
        state_b = state_b + block_ref[j, 2 * batch : 3 * batch]
        return state_f, state_b

    lax.fori_loop(0, blocks, carry, (enter_ref[0], enter_ref[1]))

    def copy(j):
        at = pl.ds(pl.multiple_of(j * rows, rows), rows)
        return pltpu.make_async_copy(out.at[:, at, :], out_hbm.at[:, at, :], out_sem.at[j])

    def step(j, _):
        at = pl.ds(pl.multiple_of(j * rows, rows), rows)
        for b in range(batch):
            out[b, at, :] = (
                mixed_ref[b, at, :]
                + from_left_ref[b, at, :] * left[j, pl.ds(b, 1), :]
                + from_right_ref[b, at, :] * right[j, pl.ds(b, 1), :]
            ).astype(BF16)
        copy(j).start()
        return _

    lax.fori_loop(0, blocks, step, 0)

    def finish(j, _):
        copy(j).wait()
        return _

    lax.fori_loop(0, blocks, finish, 0)


def per_device(n, leak_rate, signal_in, gate_in):
    batch, length, channels = leak_rate.shape
    total_length = length * n
    rows = math.gcd(length, 128)
    blocks = length // rows
    shape = (batch, length, channels)
    whole = pl.BlockSpec(memory_space=VMEM)
    far = pl.BlockSpec(memory_space=pl.ANY)
    slab = VMEM(shape, F32)
    dma = pltpu.SemaphoreType.DMA
    mixed, from_left, from_right, block, message = pl.pallas_call(
        functools.partial(local_kernel, total_length, rows),
        out_shape=(
            slab, slab, slab,
            VMEM((blocks, -(-3 * batch // 8) * 8, channels), F32),
            VMEM((2, 2 * batch, channels), F32),
        ),
        in_specs=[far] * 3,
        out_specs=(whole,) * 5,
        scratch_shapes=[
            VMEM(shape, F32), VMEM(shape, BF16), VMEM(shape, BF16),
            dma((blocks,)), dma((blocks,)), dma((blocks,)),
        ],
        compiler_params=pltpu.CompilerParams(vmem_limit_bytes=26 * MIB),
        name="local",
    )(leak_rate, signal_in, gate_in)
    enter = pl.pallas_call(
        functools.partial(exchange_kernel, total_length, n),
        out_shape=VMEM((2, batch, channels), F32),
        in_specs=[whole],
        out_specs=whole,
        scratch_shapes=[VMEM((n, 2 * batch, channels), F32), dma((n,)), dma((n,))],
        compiler_params=pltpu.CompilerParams(
            collective_id=0, has_side_effects=True, vmem_limit_bytes=4 * MIB
        ),
        name="exchange",
    )(message)
    return pl.pallas_call(
        functools.partial(finish_kernel, total_length, rows),
        out_shape=jax.ShapeDtypeStruct(shape, BF16),
        in_specs=[whole] * 5,
        out_specs=far,
        scratch_shapes=[
            VMEM(shape, BF16), VMEM((blocks, batch, channels), F32),
            VMEM((blocks, batch, channels), F32), dma((blocks,)),
        ],
        compiler_params=pltpu.CompilerParams(vmem_limit_bytes=6 * MIB),
        name="finish",
    )(mixed, from_left, from_right, block, enter)


def solution(mesh):
    spec = P(None, "sp", "tp")
    return jax.shard_map(
        functools.partial(per_device, mesh.shape["sp"]),
        mesh=mesh,
        in_specs=(spec, spec, spec),
        out_specs=spec,
        check_vma=False,
    )
```

```python
import functools
import math

import jax
import jax.numpy as jnp
from jax import lax
from jax.experimental import pallas as pl
from jax.experimental.pallas import tpu as pltpu
from jax.sharding import PartitionSpec as P

F32, BF16 = jnp.float32, jnp.bfloat16
VMEM = pltpu.VMEM
MIB = 1 << 20


def chunk_copy(hbm, vmem, sem, j, rows):
    at = pl.ds(pl.multiple_of(j * rows, rows), rows)
    return pltpu.make_async_copy(hbm.at[:, at, :], vmem.at[:, at, :], sem.at[j])


def local_kernel(
    total_length, n, rows, cols, leak_hbm, signal_hbm, gate_hbm,
    mixed_ref, from_left_ref, from_right_ref, block_ref, enter_ref,
    leak, signal, gate, message, held, leak_sem, signal_sem, gate_sem, send_sem, recv_sem,
):
    batch, length, channels = leak.shape
    blocks = length // rows
    rate = math.log2(math.e) / total_length
    half_scale = 0.5 * total_length ** -0.5
    me = lax.axis_index("sp")
    barrier = pltpu.get_barrier_semaphore()

    def start(j, _):
        chunk_copy(leak_hbm, leak, leak_sem, j, rows).start()
        chunk_copy(signal_hbm, signal, signal_sem, j, rows).start()
        return _

    def start_gate(j, _):
        chunk_copy(gate_hbm, gate, gate_sem, j, rows).start()
        return _

    ahead = math.gcd(4, blocks)
    lax.fori_loop(0, ahead, start, 0)
    for d in range(1, n):
        pl.semaphore_signal(
            barrier, inc=1, device_id={"sp": lax.rem(me + d, n)}, device_id_type=pl.DeviceIdType.MESH
        )

    row = lax.broadcasted_iota(jnp.int32, (rows, 2 * rows), 0)
    col = lax.broadcasted_iota(jnp.int32, (rows, 2 * rows), 1) % rows
    upto = jnp.where(row >= col, 1.0, 0.0).astype(BF16)
    onward = jnp.where(row <= col, 1.0, 0.0).astype(BF16)
    once = upto[:, :rows]

    def step(j, _):
        @pl.when(j + ahead < blocks)
        def more():
            start(j + ahead, 0)

        @pl.when(j + ahead >= blocks)
        def more():
            for k in range(blocks // ahead):
                start_gate((j + ahead - blocks) * (blocks // ahead) + k, 0)

        chunk_copy(leak_hbm, leak, leak_sem, j, rows).wait()
        chunk_copy(signal_hbm, signal, signal_sem, j, rows).wait()
        at = pl.ds(pl.multiple_of(j * rows, rows), rows)
        pieces = [(b, pl.ds(p, cols)) for b in range(batch) for p in range(0, channels, cols)]
        for b, cs in pieces:
            x = signal[b, at, cs]
            xf = x.astype(F32)
            a = leak[b, at, cs] * rate
            upto_here = jnp.dot(once, a.astype(BF16), preferred_element_type=F32)
            before = upto_here - a
            low_f = ((jnp.exp2(upto_here) - 1.0) * xf).astype(BF16)
            low_b = ((jnp.exp2(a - upto_here) - 1.0) * xf).astype(BF16)
            u = jnp.exp2(-upto_here)
            v = jnp.exp2(before)
            from_left_ref[b, at, cs] = u
            from_right_ref[b, at, cs] = v
            sum_f = jnp.dot(upto, jnp.concatenate([x, low_f], 0), preferred_element_type=F32)
            sum_b = jnp.dot(onward, jnp.concatenate([x, low_b], 0), preferred_element_type=F32)
            mixed_ref[b, at, cs] = u * sum_f + v * sum_b
            block_ref[j, pl.ds(b, 1), cs] = jnp.sum(a, axis=0, keepdims=True)
            block_ref[j, pl.ds(batch + b, 1), cs] = u[rows - 1 :] * sum_f[rows - 1 :]
            block_ref[j, pl.ds(2 * batch + b, 1), cs] = v[:1] * sum_b[:1]
        return _

    lax.fori_loop(0, blocks, step, 0)

    def total(k, states):
        leaked, state_f, state_b = states
        here = block_ref[k, :batch]
        state_f = jnp.exp2(-here) * state_f + block_ref[k, batch : 2 * batch]
        state_b = state_b + jnp.exp2(-leaked) * block_ref[k, 2 * batch : 3 * batch]
        return leaked + here, state_f, state_b

    zero = jnp.zeros((batch, channels), F32)
    leaked, state_f, state_b = lax.fori_loop(0, blocks, total, (zero, zero, zero))
    message[0, :batch] = leaked
    message[1, :batch] = leaked
    message[0, batch:] = state_f
    message[1, batch:] = state_b

    pl.semaphore_wait(barrier, n - 1)
    copies = []
    for d in range(1, n):
        copies.append(pltpu.make_async_remote_copy(
            src_ref=message.at[jnp.where(me + d < n, 0, 1)],
            dst_ref=held.at[d],
            send_sem=send_sem.at[d],
            recv_sem=recv_sem.at[d],
            device_id={"sp": lax.rem(me + d, n)},
            device_id_type=pl.DeviceIdType.MESH,
        ))
        copies[-1].start()

    def apply_gate(j, _):
        chunk_copy(gate_hbm, gate, gate_sem, j, rows).wait()
        at = pl.ds(pl.multiple_of(j * rows, rows), rows)
        for b in range(batch):
            open_by = half_scale + half_scale * jnp.tanh((gate[b, at, :] * 0.5).astype(F32))
            mixed_ref[b, at, :] = mixed_ref[b, at, :] * open_by
            from_left_ref[b, at, :] = from_left_ref[b, at, :] * open_by
            from_right_ref[b, at, :] = from_right_ref[b, at, :] * open_by
        return _

    lax.fori_loop(0, blocks, apply_gate, 0)
    for copy in copies:
        copy.wait()
    state_f, state_b, passed_f, passed_b = zero, zero, zero, zero
    for d in range(1, n):
        got = held[d]
        state_f = jnp.where(me >= d, state_f + jnp.exp2(-passed_f) * got[batch:], state_f)
        passed_f = passed_f + got[:batch]
        got = held[n - d]
        state_b = jnp.where(me + d < n, state_b + jnp.exp2(-passed_b) * got[batch:], state_b)
        passed_b = passed_b + got[:batch]
    enter_ref[0] = state_f
    enter_ref[1] = state_b


def finish_kernel(
    rows, mixed_ref, from_left_ref, from_right_ref, block_ref, enter_ref,
    out_hbm, out, left, right, out_sem,
):
    batch, length, channels = out.shape
    blocks = length // rows

    def carry(k, states):
        state_f, state_b = states
        left[k] = state_f
        state_f = jnp.exp2(-block_ref[k, :batch]) * state_f + block_ref[k, batch : 2 * batch]
        j = blocks - 1 - k
        state_b = jnp.exp2(-block_ref[j, :batch]) * state_b
        right[j] = state_b
        state_b = state_b + block_ref[j, 2 * batch : 3 * batch]
        return state_f, state_b

    lax.fori_loop(0, blocks, carry, (enter_ref[0], enter_ref[1]))

    def copy(j):
        at = pl.ds(pl.multiple_of(j * rows, rows), rows)
        return pltpu.make_async_copy(out.at[:, at, :], out_hbm.at[:, at, :], out_sem.at[j])

    def step(j, _):
        at = pl.ds(pl.multiple_of(j * rows, rows), rows)
        for b in range(batch):
            out[b, at, :] = (
                mixed_ref[b, at, :]
                + from_left_ref[b, at, :] * left[j, pl.ds(b, 1), :]
                + from_right_ref[b, at, :] * right[j, pl.ds(b, 1), :]
            ).astype(BF16)
        copy(j).start()
        return _

    lax.fori_loop(0, blocks, step, 0)

    def finish(j, _):
        copy(j).wait()
        return _

    lax.fori_loop(0, blocks, finish, 0)


def per_device(n, leak_rate, signal_in, gate_in):
    batch, length, channels = leak_rate.shape
    total_length = length * n
    rows = math.gcd(length, 128)
    blocks = length // rows
    shape = (batch, length, channels)
    whole = pl.BlockSpec(memory_space=VMEM)
    far = pl.BlockSpec(memory_space=pl.ANY)
    slab = VMEM(shape, F32)
    dma = pltpu.SemaphoreType.DMA
    mixed, from_left, from_right, block, enter = pl.pallas_call(
        functools.partial(local_kernel, total_length, n, rows, channels),
        out_shape=(
            slab, slab, slab,
            VMEM((blocks, -(-3 * batch // 8) * 8, channels), F32),
            VMEM((2, batch, channels), F32),
        ),
        in_specs=[far] * 3,
        out_specs=(whole,) * 5,
        scratch_shapes=[
            VMEM(shape, F32), VMEM(shape, BF16), VMEM(shape, BF16),
            VMEM((2, 2 * batch, channels), F32), VMEM((n, 2 * batch, channels), F32),
            dma((blocks,)), dma((blocks,)), dma((blocks,)), dma((n,)), dma((n,)),
        ],
        compiler_params=pltpu.CompilerParams(
            collective_id=0, has_side_effects=True, vmem_limit_bytes=26 * MIB
        ),
        name="local",
    )(leak_rate, signal_in, gate_in)
    return pl.pallas_call(
        functools.partial(finish_kernel, rows),
        out_shape=jax.ShapeDtypeStruct(shape, BF16),
        in_specs=[whole] * 5,
        out_specs=far,
        scratch_shapes=[
            VMEM(shape, BF16), VMEM((blocks, batch, channels), F32),
            VMEM((blocks, batch, channels), F32), dma((blocks,)),
        ],
        compiler_params=pltpu.CompilerParams(vmem_limit_bytes=6 * MIB),
        name="finish",
    )(mixed, from_left, from_right, block, enter)


def solution(mesh):
    spec = P(None, "sp", "tp")
    return jax.shard_map(
        functools.partial(per_device, mesh.shape["sp"]),
        mesh=mesh,
        in_specs=(spec, spec, spec),
        out_specs=spec,
        check_vma=False,
    )
```
